32 devices in a mesh: dp: 1 (over z), tp: 32 (over x, y, core).
Axes of the slice: x: 4, y: 4, z: 1, core: 2. Of those that a mesh axis runs over, the one named last changes fastest.
The devices are a block of a 4x4x8 slice.
Arguments:
- x: bfloat16 [2048, 5120], P('dp')
- w_gate: bfloat16 [5120, 16384], P(None, 'tp')
- w_up: bfloat16 [5120, 16384], P(None, 'tp')
- w_down: bfloat16 [16384, 5120], P('tp')
Outputs:
- output: bfloat16 [2048, 5120], P('dp')
All inputs are finite; a program needn't handle non-finite values.
Results may differ from the reference program's by a relative error of at most 0.016.
Values are sent between devices in bfloat16 or wider.
A program may use at most 768 MiB of HBM per device.

```python
import jax
import jax.numpy as jnp

ROWS = 2048
D = 5120
FF = 16384


def setup_inputs(seed: int = 0, part: int = 0) -> dict:
    kx, kg, ku, kd = jax.random.split(jax.random.key(seed), 4)
    drawn = {
        "x": jax.random.normal(jax.random.fold_in(kx, part), (ROWS, D), jnp.float32),
        "w_gate": jax.random.normal(kg, (D, FF), jnp.float32) * D**-0.5,
        "w_up": jax.random.normal(ku, (D, FF), jnp.float32) * D**-0.5,
        "w_down": jax.random.normal(kd, (FF, D), jnp.float32) * FF**-0.5,
    }
    return {k: v.astype(jnp.bfloat16) for k, v in drawn.items()}


def reference(x, w_gate, w_up, w_down):
    gate = jnp.dot(x, w_gate, preferred_element_type=jnp.float32)
    up = jnp.dot(x, w_up, preferred_element_type=jnp.float32)
    hidden = (jax.nn.silu(gate) * up).astype(jnp.bfloat16)
    return jnp.dot(hidden, w_down, preferred_element_type=jnp.float32).astype(jnp.bfloat16)
```

```python
import functools
import math

import jax
import jax.numpy as jnp
from jax import lax
from jax.experimental import pallas as pl
from jax.experimental.pallas import tpu as pltpu
from jax.sharding import PartitionSpec as P

MESH = pl.DeviceIdType.MESH
ROWS = 128
KSLICES = 5
F32, BF16 = jnp.float32, jnp.bfloat16


def _kernel(
    side, nc, x_hbm, wg_hbm, wu_hbm, wd_hbm, y,
    wg, wu, wd, xb, h, p32, p16, got1, got2, fw1, fw2, t32, t16,
    s1, r1, s2, r2, sg2, rg2, sg1, rg1, sd, rd, sh, rh, swd, rwd, lx, lw, lwd,
):
    R = xb.shape[1]
    K = xb.shape[2]
    FF = wg.shape[1]
    C = p32.shape[2]
    CB, CH = C // 2, C // 4
    R1, R2 = R // side, R // side // side

    me = lax.axis_index("tp")
    core = lax.rem(me, 2)
    chip = lax.div(me, 2)
    cx, cy = lax.div(chip, side), lax.rem(chip, side)
    mate = me + 1 - 2 * core

    def dev(a, b):
        return (lax.rem(a + side, side) * side + lax.rem(b + side, side)) * 2 + core

    xp, xm, yp, ym = dev(cx + 1, cy), dev(cx - 1, cy), dev(cx, cy + 1), dev(cx, cy - 1)
    ring = {
        1: ((cx, xp, xm), (cy, yp, ym)),
        2: ((cy, yp, ym), (cx, xp, xm)),
    }

    def remote(src, dst, ssem, rsem, to):
        return pltpu.make_async_remote_copy(
            src_ref=src, dst_ref=dst, send_sem=ssem, recv_sem=rsem,
            device_id={"tp": to}, device_id_type=MESH,
        )

    def load_x(j):
        rows = pl.ds(pl.multiple_of(j * R, R), R)
        slot = lax.rem(j, 2)
        return pltpu.make_async_copy(x_hbm.at[rows, :], xb.at[slot], lx.at[slot])

    KS = K // KSLICES

    def load_w(i):
        rows = pl.ds(i * KS, KS)
        return (
            pltpu.make_async_copy(wg_hbm.at[rows, :], wg.at[rows, :], lw.at[0, i]),
            pltpu.make_async_copy(wu_hbm.at[rows, :], wu.at[rows, :], lw.at[1, i]),
        )

    my_cols = pl.ds(pl.multiple_of(core * C, C), C)
    mate_cols = pl.ds(pl.multiple_of((1 - core) * C, C), C)

    load_x(0).start()
    for i in range(KSLICES):
        for copy in load_w(i):
            copy.start()
    wd_own = pltpu.make_async_copy(wd_hbm.at[:, my_cols], wd.at[pl.ds(0, FF), :], lwd)
    wd_own.start()
    load_x(1).start()

    barrier = pltpu.get_barrier_semaphore()
    for d in (mate, xp, xm, yp, ym):
        pl.semaphore_signal(barrier, inc=1, device_id={"tp": d}, device_id_type=MESH)
    pl.semaphore_wait(barrier, 5)

    wd_mate = remote(wd_hbm.at[:, mate_cols], wd.at[pl.ds(FF, FF), :], swd, rwd, mate)
    wd_mate.start()

    def send_h(j):
        return remote(
            h.at[j, :, pl.ds(0, FF)], h.at[j, :, pl.ds(FF, FF)], sh.at[j], rh.at[j], mate
        )

    TN = min(256, FF)

    def gate_up(j):
        slot = lax.rem(j, 2)
        load_x(j).wait()
        for t in range(FF // TN):
            cols = pl.ds(t * TN, TN)
            g = jnp.dot(xb[slot], wg[:, cols], preferred_element_type=F32)
            u = jnp.dot(xb[slot], wu[:, cols], preferred_element_type=F32)
            h[j, :, cols] = (jax.nn.silu(g) * u).astype(BF16)
        send_h(j).start()

        @pl.when(j + 2 < nc)
        def _():
            load_x(j + 2).start()

    def gate_up_first():
        load_x(0).wait()
        for i in range(KSLICES):
            for copy in load_w(i):
                copy.wait()
            part = pl.ds(i * KS, KS)
            g = jnp.dot(xb[0, :, part], wg[part, :], preferred_element_type=F32)
            u = jnp.dot(xb[0, :, part], wu[part, :], preferred_element_type=F32)
            if i > 0:
                g, u = p32[0, :, pl.ds(0, FF)] + g, p32[1, :, pl.ds(0, FF)] + u
            if i < KSLICES - 1:
                p32[0, :, pl.ds(0, FF)] = g
                p32[1, :, pl.ds(0, FF)] = u
            else:
                h[0, :, pl.ds(0, FF)] = (jax.nn.silu(g) * u).astype(BF16)
        send_h(0).start()
        load_x(2).start()

    TD = 512 if C % 512 == 0 else CH

    def down(j):
        slot = lax.rem(j, 2)
        send_h(j).wait()
        for t in range(C // TD):
            cols = pl.ds(t * TD, TD)
            p = jnp.dot(h[j], wd[:, cols], preferred_element_type=F32)
            p32[slot, :, cols] = p
            p16[slot, :, cols] = p.astype(BF16)

    def piece(phase, q):
        size = R1 if phase == 1 else R2
        return pl.ds(pl.multiple_of(lax.rem(q + side, side) * size, size), size)

    def half(phase, k, hf):
        return pl.ds((k * CB if phase == 1 else 0) + hf * CH, CH)

    def term(phase, j, k, q, hf, wide):
        slot = lax.rem(j, 2)
        where = (piece(phase, q), half(phase, k, hf))
        if phase == 1:
            return (p32 if wide else p16).at[slot, *where]
        return (t32 if wide else t16).at[slot, k, *where]

    bufs = {1: (got1, fw1, s1, r1), 2: (got2, fw2, s2, r2)}

    def message(phase, j, k, m):
        got, fw, ss, rs = bufs[phase]
        q, np_, nm = ring[phase][k]
        slot = lax.rem(j, 2)
        if m < 4:
            dq, hf, to = ((2, 0, np_), (2, 1, nm), (1, 1, np_), (-1, 0, nm))[m]
            src = term(phase, j, k, q + dq, hf, False)
        else:
            src, to = fw.at[slot, k, m - 4], (np_, nm)[m - 4]
        return remote(src, got.at[j, k, m], ss.at[slot, k, m], rs.at[j, k, m], to)

    def rs_raw(phase, j):
        for m in range(4):
            for k in range(2):
                message(phase, j, k, m).start()

    def rs_forward(phase, j):
        got, fw, _, _ = bufs[phase]
        slot = lax.rem(j, 2)
        for hf in range(2):
            for k in range(2):
                q, _, _ = ring[phase][k]
                message(phase, j, k, hf).wait_recv()
                qq = q + 1 if hf == 0 else q - 1
                total = term(phase, j, k, qq, hf, True)[...] + got[j, k, hf].astype(F32)
                fw[slot, k, hf] = total.astype(BF16)
                message(phase, j, k, 4 + hf).start()

    def rs_finish(phase, j, store):
        got, _, _, _ = bufs[phase]
        for k in range(2):
            q, _, _ = ring[phase][k]
            for hf in range(2):
                message(phase, j, k, 4 + hf).wait_recv()
                message(phase, j, k, 3 - hf).wait_recv()
                total = (
                    term(phase, j, k, q, hf, True)[...]
                    + got[j, k, 4 + hf].astype(F32)
                    + got[j, k, 3 - hf].astype(F32)
                )
                store(k, hf, total)
        for k in range(2):
            for m in range(6):
                message(phase, j, k, m).wait_send()

    def store_t(j):
        slot = lax.rem(j, 2)

        def store(k, hf, total):
            t32[slot, k, :, pl.ds(hf * CH, CH)] = total
            t16[slot, k, :, pl.ds(hf * CH, CH)] = total.astype(BF16)

        return store

    def y_block(phase, j, k, q, hf=None):
        q1 = ring[1][k][0]
        col = core * C + k * CB + (0 if hf is None else hf * CH)
        cols = pl.ds(pl.multiple_of(col, CH), CB if hf is None else CH)
        if phase == 2:
            row = j * R + q1 * R1 + lax.rem(q + side, side) * R2
            return y.at[pl.ds(pl.multiple_of(row, R2), R2), cols]
        row = j * R + lax.rem(q + side, side) * R1
        return y.at[pl.ds(pl.multiple_of(row, R1), R1), cols]

    gsem = {1: (sg1, rg1), 2: (sg2, rg2)}

    def gather(phase, j, k, m, got):
        ss, rs = gsem[phase]
        q, np_, nm = ring[phase][k]
        dq, hf = (((-1, None), (1, None), (-2, 0), (2, 1)) if got else ((0, None), (0, None), (-1, 0), (1, 1)))[m]
        block = y_block(phase, j, k, q + dq, hf)
        return remote(block, block, ss.at[lax.rem(j, 2), k, m], rs.at[j, k, m], (np_, nm)[m % 2])

    def ag_start(phase, j):
        for m in range(2):
            for k in range(2):
                gather(phase, j, k, m, False).start()

    def ag_pass(phase, j):
        for m in range(2):
            for k in range(2):
                gather(phase, j, k, m, True).wait_recv()
                gather(phase, j, k, 2 + m, False).start()

    def ag_end(phase, j):
        for m in range(2, 4):
            for k in range(2):
                gather(phase, j, k, m, True).wait_recv()
        for k in range(2):
            for m in range(4):
                gather(phase, j, k, m, False).wait_send()

    def swap(j, mine):
        rows = pl.ds(pl.multiple_of(j * R, R), R)
        block = y.at[rows, my_cols if mine else mate_cols]
        return remote(block, block, sd.at[lax.rem(j, 2)], rd.at[j], mate)

    def stage2(j):
        rs_finish(1, j, store_t(j))
        rs_raw(2, j)

    def stage4(j):
        def store(k, hf, total):
            q2 = ring[2][k][0]
            y_block(2, j, k, q2, hf)[...] = total.astype(BF16)

        rs_finish(2, j, store)
        ag_start(2, j)

    def stage6(j):
        ag_end(2, j)
        ag_start(1, j)

    def stage8(j):
        ag_end(1, j)
        swap(j, True).start()

    def stage9(j):
        swap(j, True).wait_send()
        swap(j, False).wait_recv()

    stages = (
        None,
        functools.partial(rs_forward, 1),
        stage2,
        functools.partial(rs_forward, 2),
        stage4,
        functools.partial(ag_pass, 2),
        stage6,
        functools.partial(ag_pass, 1),
        stage8,
        stage9,
    )

    gate_up_first()
    wd_own.wait()
    wd_mate.wait()

    def step(s, carry):
        for lag in range(len(stages) - 1, 0, -1):
            j = s - lag

            @pl.when(jnp.logical_and(j >= 0, j < nc))
            def _():
                stages[lag](j)

        @pl.when(s < nc)
        def _():
            down(s)
            rs_raw(1, s)

        @pl.when(s + 1 < nc)
        def _():
            gate_up(s + 1)

        return carry

    lax.fori_loop(0, nc + len(stages) - 1, step, 0)


def _mlp(side, x, w_gate, w_up, w_down):
    rows, depth = x.shape
    ff = w_gate.shape[1]
    width = w_down.shape[1]
    C = width // 2
    R = ROWS
    nc = rows // R
    CB, CH = C // 2, C // 4
    R1, R2 = R // side, R // side // side
    dma = pltpu.SemaphoreType.DMA
    y = pl.pallas_call(
        functools.partial(_kernel, side, nc),
        out_shape=pltpu.VMEM((rows, width), BF16),
        in_specs=[pl.BlockSpec(memory_space=pl.ANY)] * 4,
        out_specs=pl.BlockSpec(memory_space=pltpu.VMEM),
        scratch_shapes=[
            pltpu.VMEM((depth, ff), BF16),
            pltpu.VMEM((depth, ff), BF16),
            pltpu.VMEM((2 * ff, C), BF16),
            pltpu.VMEM((2, R, depth), BF16),
            pltpu.VMEM((nc, R, 2 * ff), BF16),
            pltpu.VMEM((2, R, C), F32),
            pltpu.VMEM((2, R, C), BF16),
            pltpu.VMEM((nc, 2, 6, R1, CH), BF16),
            pltpu.VMEM((nc, 2, 6, R2, CH), BF16),
            pltpu.VMEM((2, 2, 2, R1, CH), BF16),
            pltpu.VMEM((2, 2, 2, R2, CH), BF16),
            pltpu.VMEM((2, 2, R1, CB), F32),
            pltpu.VMEM((2, 2, R1, CB), BF16),
            dma((2, 2, 6)), dma((nc, 2, 6)),
            dma((2, 2, 6)), dma((nc, 2, 6)),
            dma((2, 2, 4)), dma((nc, 2, 4)),
            dma((2, 2, 4)), dma((nc, 2, 4)),
            dma((2,)), dma((nc,)),
            dma((nc,)), dma((nc,)),
            dma, dma,
            dma((2,)), dma((2, KSLICES)), dma,
        ],
        compiler_params=pltpu.CompilerParams(
            collective_id=0, has_side_effects=True, vmem_limit_bytes=43 * 1024 * 1024,
        ),
        cost_estimate=pl.CostEstimate(
            flops=6 * rows * depth * ff, bytes_accessed=4 * rows * depth, transcendentals=rows * ff,
        ),
    )(x, w_gate, w_up, w_down)
    return y


def solution(mesh):
    side = math.isqrt(mesh.shape["tp"] // 2)

    return jax.shard_map(
        functools.partial(_mlp, side),
        mesh=mesh,
        in_specs=(P("dp", None), P(None, "tp"), P(None, "tp"), P("tp", None)),
        out_specs=P("dp", None),
        check_vma=False,
    )
```

```python
import functools
import math

import jax
import jax.numpy as jnp
from jax import lax
from jax.experimental import pallas as pl
from jax.experimental.pallas import tpu as pltpu
from jax.sharding import PartitionSpec as P

MESH = pl.DeviceIdType.MESH
ROWS = 128
KSLICES = 5
LAGS = (0, 2, 4, 6, 8, 10, 14, 16, 18, 20)
SLOTS = 8
F32, BF16 = jnp.float32, jnp.bfloat16


def _kernel(
    side, nc, x_hbm, wg_hbm, wu_hbm, wd_hbm, y,
    wg, wu, wd, xb, h, p32, p16, got1, got2, fw1, fw2, t32, t16,
    s1a, s1b, r1a, r1b, s2a, s2b, r2a, r2b, sg2a, sg2b, rg2a, rg2b, sg1a, sg1b, rg1a, rg1b, sd, rd, sh, rh, swd, rwd, lx, lw, lwd,
):
    R = xb.shape[1]
    K = xb.shape[2]
    FF = wg.shape[1]
    C = p32.shape[2]
    CB, CH = C // 2, C // 4
    R1, R2 = R // side, R // side // side

    me = lax.axis_index("tp")
    core = lax.rem(me, 2)
    chip = lax.div(me, 2)
    cx, cy = lax.div(chip, side), lax.rem(chip, side)
    mate = me + 1 - 2 * core

    def dev(a, b):
        return (lax.rem(a + side, side) * side + lax.rem(b + side, side)) * 2 + core

    xp, xm, yp, ym = dev(cx + 1, cy), dev(cx - 1, cy), dev(cx, cy + 1), dev(cx, cy - 1)
    ring = {
        1: ((cx, xp, xm), (cy, yp, ym)),
        2: ((cy, yp, ym), (cx, xp, xm)),
    }

    def remote(src, dst, ssem, rsem, to):
        return pltpu.make_async_remote_copy(
            src_ref=src, dst_ref=dst, send_sem=ssem, recv_sem=rsem,
            device_id={"tp": to}, device_id_type=MESH,
        )

    def turn(ref, j):
        return lax.rem(j, ref.shape[0])

    def load_x(j):
        rows = pl.ds(pl.multiple_of(j * R, R), R)
        slot = lax.rem(j, 2)
        return pltpu.make_async_copy(x_hbm.at[rows, :], xb.at[slot], lx.at[slot])

    KS = K // KSLICES

    def load_w(i):
        rows = pl.ds(i * KS, KS)
        return (
            pltpu.make_async_copy(wg_hbm.at[rows, :], wg.at[rows, :], lw.at[0, i]),
            pltpu.make_async_copy(wu_hbm.at[rows, :], wu.at[rows, :], lw.at[1, i]),
        )

    my_cols = pl.ds(pl.multiple_of(core * C, C), C)
    mate_cols = pl.ds(pl.multiple_of((1 - core) * C, C), C)

    load_x(0).start()
    for i in range(KSLICES):
        for copy in load_w(i):
            copy.start()
    wd_own = pltpu.make_async_copy(wd_hbm.at[:, my_cols], wd.at[pl.ds(0, FF), :], lwd)
    wd_own.start()
    load_x(1).start()

    barrier = pltpu.get_barrier_semaphore()
    for d in (mate, xp, xm, yp, ym):
        pl.semaphore_signal(barrier, inc=1, device_id={"tp": d}, device_id_type=MESH)
    pl.semaphore_wait(barrier, 5)

    wd_mate = remote(wd_hbm.at[:, mate_cols], wd.at[pl.ds(FF, FF), :], swd, rwd, mate)
    wd_mate.start()

    def send_h(j):
        return remote(
            h.at[turn(h, j), :, pl.ds(0, FF)], h.at[turn(h, j), :, pl.ds(FF, FF)],
            sh.at[turn(sh, j)], rh.at[turn(rh, j)], mate,
        )

    TN = min(256, FF)

    def gate_up(j):
        slot = lax.rem(j, 2)
        load_x(j).wait()
        for t in range(FF // TN):
            cols = pl.ds(t * TN, TN)
            g = jnp.dot(xb[slot], wg[:, cols], preferred_element_type=F32)
            u = jnp.dot(xb[slot], wu[:, cols], preferred_element_type=F32)
            h[turn(h, j), :, cols] = (jax.nn.silu(g) * u).astype(BF16)
        send_h(j).start()

        @pl.when(j + 2 < nc)
        def _():
            load_x(j + 2).start()

    def gate_up_first():
        load_x(0).wait()
        for i in range(KSLICES):
            for copy in load_w(i):
                copy.wait()
            part = pl.ds(i * KS, KS)
            g = jnp.dot(xb[0, :, part], wg[part, :], preferred_element_type=F32)
            u = jnp.dot(xb[0, :, part], wu[part, :], preferred_element_type=F32)
            if i > 0:
                g, u = p32[0, :, pl.ds(0, FF)] + g, p32[1, :, pl.ds(0, FF)] + u
            if i < KSLICES - 1:
                p32[0, :, pl.ds(0, FF)] = g
                p32[1, :, pl.ds(0, FF)] = u
            else:
                h[0, :, pl.ds(0, FF)] = (jax.nn.silu(g) * u).astype(BF16)
        send_h(0).start()
        load_x(2).start()

    TD = 512 if C % 512 == 0 else CH

    def down(j):
        send_h(j).wait()
        for t in range(C // TD):
            cols = pl.ds(t * TD, TD)
            p = jnp.dot(h[turn(h, j)], wd[:, cols], preferred_element_type=F32)
            p32[turn(p32, j), :, cols] = p
            p16[turn(p16, j), :, cols] = p.astype(BF16)

    def piece(phase, q):
        size = R1 if phase == 1 else R2
        return pl.ds(pl.multiple_of(lax.rem(q + side, side) * size, size), size)

    def half(phase, k, hf):
        return pl.ds((k * CB if phase == 1 else 0) + hf * CH, CH)

    def term(phase, j, k, q, hf, wide):
        where = (piece(phase, q), half(phase, k, hf))
        if phase == 1:
            ref = p32 if wide else p16
            return ref.at[turn(ref, j), *where]
        ref = t32 if wide else t16
        return ref.at[turn(ref, j), k, *where]

    bufs = {1: (got1, fw1, (s1a, s1b), (r1a, r1b)), 2: (got2, fw2, (s2a, s2b), (r2a, r2b))}

    def message(phase, j, k, m):
        got, fw, ss, rs = bufs[phase]
        q, np_, nm = ring[phase][k]
        if m < 4:
            dq, hf, to = ((2, 0, np_), (2, 1, nm), (1, 1, np_), (-1, 0, nm))[m]
            src = term(phase, j, k, q + dq, hf, False)
        else:
            src, to = fw.at[turn(fw, j), k, m - 4], (np_, nm)[m - 4]
        return remote(
            src, got.at[turn(got, j), m, k],
            ss[m // 4].at[turn(ss[m // 4], j)], rs[m // 2 > 0].at[turn(rs[m // 2 > 0], j)], to,
        )

    def messages(phase, j, lo, hi):
        got, _, ss, rs = bufs[phase]
        block = got.at[turn(got, j), pl.ds(lo, hi - lo)]
        return remote(block, block, ss[lo // 4].at[turn(ss[lo // 4], j)], rs[lo // 2 > 0].at[turn(rs[lo // 2 > 0], j)], mate)

    def rs_raw(phase, j):
        for m in range(4):
            for k in range(2):
                message(phase, j, k, m).start()

    def rs_forward(phase, j):
        got, fw, _, _ = bufs[phase]
        messages(phase, j, 0, 2).wait_recv()
        for hf in range(2):
            for k in range(2):
                q, _, _ = ring[phase][k]
                qq = q + 1 if hf == 0 else q - 1
                total = term(phase, j, k, qq, hf, True)[...] + got[turn(got, j), hf, k].astype(F32)
                fw[turn(fw, j), k, hf] = total.astype(BF16)
                message(phase, j, k, 4 + hf).start()
        messages(phase, j, 0, 4).wait_send()

    def rs_finish(phase, j, store):
        got, _, _, _ = bufs[phase]
        messages(phase, j, 2, 6).wait_recv()
        for k in range(2):
            q, _, _ = ring[phase][k]
            for hf in range(2):
                total = (
                    term(phase, j, k, q, hf, True)[...]
                    + got[turn(got, j), 4 + hf, k].astype(F32)
                    + got[turn(got, j), 3 - hf, k].astype(F32)
                )
                store(k, hf, total)
        messages(phase, j, 4, 6).wait_send()

    def store_t(j):
        def store(k, hf, total):
            t32[turn(t32, j), k, :, pl.ds(hf * CH, CH)] = total
            t16[turn(t16, j), k, :, pl.ds(hf * CH, CH)] = total.astype(BF16)

        return store

    def y_block(phase, j, k, q, hf=None):
        q1 = ring[1][k][0]
        col = core * C + k * CB + (0 if hf is None else hf * CH)
        cols = pl.ds(pl.multiple_of(col, CH), CB if hf is None else CH)
        if phase == 2:
            row = j * R + q1 * R1 + lax.rem(q + side, side) * R2
            return y.at[pl.ds(pl.multiple_of(row, R2), R2), cols]
        row = j * R + lax.rem(q + side, side) * R1
        return y.at[pl.ds(pl.multiple_of(row, R1), R1), cols]

    gsem = {1: ((sg1a, sg1b), (rg1a, rg1b)), 2: ((sg2a, sg2b), (rg2a, rg2b))}

    def gather(phase, j, k, m):
        ss, rs = (sems[m // 2] for sems in gsem[phase])
        q, np_, nm = ring[phase][k]
        dq, hf = ((0, None), (0, None), (-1, 0), (1, 1))[m]
        block = y_block(phase, j, k, q + dq, hf)
        return remote(block, block, ss.at[turn(ss, j)], rs.at[turn(rs, j)], (np_, nm)[m % 2])

    def gathers(phase, j, late):
        ss, rs = (sems[late] for sems in gsem[phase])
        size = (R1, R)[phase == 1] // (1 + late)
        block = y.at[pl.ds(pl.multiple_of(j * R, R), size), pl.ds(0, CB)]
        return remote(block, block, ss.at[turn(ss, j)], rs.at[turn(rs, j)], mate)

    def ag_start(phase, j):
        for m in range(2):
            for k in range(2):
                gather(phase, j, k, m).start()

    def ag_pass(phase, j):
        gathers(phase, j, 0).wait_recv()
        for m in range(2):
            for k in range(2):
                gather(phase, j, k, 2 + m).start()
        gathers(phase, j, 0).wait_send()

    def ag_end(phase, j):
        gathers(phase, j, 1).wait_recv()
        gathers(phase, j, 1).wait_send()

    def swap(j, mine):
        rows = pl.ds(pl.multiple_of(j * R, R), R)
        block = y.at[rows, my_cols if mine else mate_cols]
        return remote(block, block, sd.at[turn(sd, j)], rd.at[turn(rd, j)], mate)

    def stage2(j):
        rs_finish(1, j, store_t(j))
        rs_raw(2, j)

    def stage4(j):
        def store(k, hf, total):
            q2 = ring[2][k][0]
            y_block(2, j, k, q2, hf)[...] = total.astype(BF16)

        rs_finish(2, j, store)
        ag_start(2, j)

    def stage6(j):
        ag_end(2, j)
        ag_start(1, j)

    def stage8(j):
        ag_end(1, j)
        swap(j, True).start()

    def stage9(j):
        swap(j, True).wait_send()
        swap(j, False).wait_recv()

    stages = (
        None,
        functools.partial(rs_forward, 1),
        stage2,
        functools.partial(rs_forward, 2),
        stage4,
        functools.partial(ag_pass, 2),
        stage6,
        functools.partial(ag_pass, 1),
        stage8,
        stage9,
    )

    gate_up_first()
    wd_own.wait()
    wd_mate.wait()

    def step(s, carry):
        for i in range(len(stages) - 1, 0, -1):
            j = s - LAGS[i]

            @pl.when(jnp.logical_and(j >= 0, j < nc))
            def _():
                stages[i](j)

        @pl.when(s + 1 < nc)
        def _():
            gate_up(s + 1)

        @pl.when(s < nc)
        def _():
            down(s)
            rs_raw(1, s)

        return carry

    lax.fori_loop(0, nc + LAGS[-1], step, 0)


def _mlp(side, x, w_gate, w_up, w_down):
    rows, depth = x.shape
    ff = w_gate.shape[1]
    width = w_down.shape[1]
    C = width // 2
    R = ROWS
    nc = rows // R
    CB, CH = C // 2, C // 4
    R1, R2 = R // side, R // side // side
    L = LAGS
    dma = pltpu.SemaphoreType.DMA
    y = pl.pallas_call(
        functools.partial(_kernel, side, nc),
        out_shape=pltpu.VMEM((rows, width), BF16),
        in_specs=[pl.BlockSpec(memory_space=pl.ANY)] * 4,
        out_specs=pl.BlockSpec(memory_space=pltpu.VMEM),
        scratch_shapes=[
            pltpu.VMEM((depth, ff), BF16),
            pltpu.VMEM((depth, ff), BF16),
            pltpu.VMEM((2 * ff, C), BF16),
            pltpu.VMEM((2, R, depth), BF16),
            pltpu.VMEM((4, R, 2 * ff), BF16),
            pltpu.VMEM((L[2], R, C), F32),
            pltpu.VMEM((L[1], R, C), BF16),
            pltpu.VMEM((SLOTS, 6, 2, R1, CH), BF16),
            pltpu.VMEM((SLOTS, 6, 2, R2, CH), BF16),
            pltpu.VMEM((L[2] - L[1], 2, 2, R1, CH), BF16),
            pltpu.VMEM((L[4] - L[3], 2, 2, R2, CH), BF16),
            pltpu.VMEM((L[4] - L[2], 2, R1, CB), F32),
            pltpu.VMEM((L[3] - L[2], 2, R1, CB), BF16),
            dma((L[1],)), dma((L[2] - L[1],)), dma((SLOTS,)), dma((SLOTS,)),
            dma((L[3] - L[2],)), dma((L[4] - L[3],)), dma((SLOTS,)), dma((SLOTS,)),
            dma((L[5] - L[4],)), dma((L[6] - L[5],)), dma((SLOTS,)), dma((SLOTS,)),
            dma((L[7] - L[6],)), dma((L[8] - L[7],)), dma((SLOTS,)), dma((SLOTS,)),
            dma((L[9] - L[8],)), dma((SLOTS,)),
            dma((2,)), dma((4,)),
            dma, dma,
            dma((2,)), dma((2, KSLICES)), dma,
        ],
        compiler_params=pltpu.CompilerParams(
            collective_id=0, has_side_effects=True, vmem_limit_bytes=43 * 1024 * 1024,
        ),
        cost_estimate=pl.CostEstimate(
            flops=6 * rows * depth * ff, bytes_accessed=4 * rows * depth, transcendentals=rows * ff,
        ),
    )(x, w_gate, w_up, w_down)
    return y


def solution(mesh):
    side = math.isqrt(mesh.shape["tp"] // 2)

    return jax.shard_map(
        functools.partial(_mlp, side),
        mesh=mesh,
        in_specs=(P("dp", None), P(None, "tp"), P(None, "tp"), P("tp", None)),
        out_specs=P("dp", None),
        check_vma=False,
    )
```

```python
import functools
import math

import jax
import jax.numpy as jnp
from jax import lax
from jax.experimental import pallas as pl
from jax.experimental.pallas import tpu as pltpu
from jax.sharding import PartitionSpec as P

MESH = pl.DeviceIdType.MESH
ROWS = 128
STORES = 8
AHEAD = 4
MATE_AT = 0
KSLICES = 10
LAGS = (0, 2, 4, 6, 8, 10, 14, 19, 25, 27)
F32, BF16 = jnp.float32, jnp.bfloat16


def _kernel(
    side, nc, x_hbm, wg_hbm, wu_hbm, wd_hbm, y,
    w, wd, xb, h, p32, p16, got1, got2, fw1, fw2, t32, t16,
    s1a, s1b, r1a, r1b, s2a, s2b, r2a, r2b, sg2a, sg2b, rg2a, rg2b, sg1a, sg1b, rg1a, rg1b, sd, rd, sh, rh, swd, rwd, lx, lw, lwd,
):
    R = xb.shape[1]
    K = xb.shape[2]
    FF = w.shape[2]
    C = p32.shape[2]
    CB, CH = C // 2, C // 4
    R1, R2 = R // side, R // side // side

    me = lax.axis_index("tp")
    core = lax.rem(me, 2)
    chip = lax.div(me, 2)
    cx, cy = lax.div(chip, side), lax.rem(chip, side)
    mate = me + 1 - 2 * core

    def dev(a, b):
        return (lax.rem(a + side, side) * side + lax.rem(b + side, side)) * 2 + core

    xp, xm, yp, ym = dev(cx + 1, cy), dev(cx - 1, cy), dev(cx, cy + 1), dev(cx, cy - 1)
    ring = {
        1: ((cx, xp, xm), (cy, yp, ym)),
        2: ((cy, yp, ym), (cx, xp, xm)),
    }

    def remote(src, dst, ssem, rsem, to):
        return pltpu.make_async_remote_copy(
            src_ref=src, dst_ref=dst, send_sem=ssem, recv_sem=rsem,
            device_id={"tp": to}, device_id_type=MESH,
        )

    def turn(ref, j):
        return lax.rem(j, ref.shape[0])

    def load_x(j):
        rows = pl.ds(pl.multiple_of(j * R, R), R)
        slot = lax.rem(j, 2)
        return pltpu.make_async_copy(x_hbm.at[rows, :], xb.at[slot], lx.at[slot])

    KS = K // KSLICES

    def load_w(i):
        rows = pl.ds(i * KS, KS)
        return (
            pltpu.make_async_copy(wg_hbm.at[rows, :], w.at[0, rows, :], lw.at[i % AHEAD]),
            pltpu.make_async_copy(wu_hbm.at[rows, :], w.at[1, rows, :], lw.at[i % AHEAD]),
        )

    my_cols = pl.ds(pl.multiple_of(core * C, C), C)
    mate_cols = pl.ds(pl.multiple_of((1 - core) * C, C), C)

    load_x(0).start()
    for i in range(AHEAD):
        for copy in load_w(i):
            copy.start()
    wd_own = pltpu.make_async_copy(wd_hbm.at[:, my_cols], wd.at[pl.ds(0, FF), :], lwd)

    barrier = pltpu.get_barrier_semaphore()
    for d in (mate, xp, xm, yp, ym):
        pl.semaphore_signal(barrier, inc=1, device_id={"tp": d}, device_id_type=MESH)
    pl.semaphore_wait(barrier, 5)

    wd_mate = remote(wd_hbm.at[:, mate_cols], wd.at[pl.ds(FF, FF), :], swd, rwd, mate)

    def send_h(j):
        return remote(
            h.at[turn(h, j), :, pl.ds(0, FF)], h.at[turn(h, j), :, pl.ds(FF, FF)],
            sh.at[turn(sh, j)], rh.at[turn(rh, j)], mate,
        )

    TN = min(256, FF)

    def gate_up(j):
        slot = lax.rem(j, 2)
        load_x(j).wait()
        for t in range(FF // TN):
            cols = pl.ds(t * TN, TN)
            g = jnp.dot(xb[slot], w[0, :, cols], preferred_element_type=F32)
            u = jnp.dot(xb[slot], w[1, :, cols], preferred_element_type=F32)
            h[turn(h, j), :, cols] = (jax.nn.silu(g) * u).astype(BF16)
        send_h(j).start()

        @pl.when(j + 2 < nc)
        def _():
            load_x(j + 2).start()

    def gate_up_first():
        load_x(0).wait()
        for i in range(KSLICES):
            part = pl.ds(i * KS, KS)
            pltpu.make_async_copy(w.at[:, part, :], w.at[:, part, :], lw.at[i % AHEAD]).wait()
            if i == MATE_AT:
                wd_mate.start()
            if i + AHEAD < KSLICES:
                for copy in load_w(i + AHEAD):
                    copy.start()
            elif i + AHEAD == KSLICES:
                load_x(1).start()
                wd_own.start()
            g = jnp.dot(xb[0, :, part], w[0, part, :], preferred_element_type=F32)
            u = jnp.dot(xb[0, :, part], w[1, part, :], preferred_element_type=F32)
            if i > 0:
                g, u = p32[0, :, pl.ds(0, FF)] + g, p32[1, :, pl.ds(0, FF)] + u
            if i < KSLICES - 1:
                p32[0, :, pl.ds(0, FF)] = g
                p32[1, :, pl.ds(0, FF)] = u
            else:
                h[0, :, pl.ds(0, FF)] = (jax.nn.silu(g) * u).astype(BF16)
        send_h(0).start()
        load_x(2).start()

    TD = 512 if C % 512 == 0 else CH

    def down(j):
        send_h(j).wait()
        for t in range(C // TD):
            cols = pl.ds(t * TD, TD)
            p = jnp.dot(h[turn(h, j)], wd[:, cols], preferred_element_type=F32)
            p32[turn(p32, j), :, cols] = p
            p16[turn(p16, j), :, cols] = p.astype(BF16)

    def piece(phase, q):
        size = R1 if phase == 1 else R2
        return pl.ds(pl.multiple_of(lax.rem(q + side, side) * size, size), size)

    def half(phase, k, hf):
        return pl.ds((k * CB if phase == 1 else 0) + hf * CH, CH)

    def term(phase, j, k, q, hf, wide):
        where = (piece(phase, q), half(phase, k, hf))
        if phase == 1:
            ref = p32 if wide else p16
            return ref.at[turn(ref, j), *where]
        ref = t32 if wide else t16
        return ref.at[turn(ref, j), k, *where]

    bufs = {1: (got1, fw1, (s1a, s1b), (r1a, r1b)), 2: (got2, fw2, (s2a, s2b), (r2a, r2b))}

    def message(phase, j, k, m):
        got, fw, ss, rs = bufs[phase]
        q, np_, nm = ring[phase][k]
        if m < 4:
            dq, hf, to = ((2, 0, np_), (2, 1, nm), (1, 1, np_), (-1, 0, nm))[m]
            src = term(phase, j, k, q + dq, hf, False)
        else:
            src, to = fw.at[turn(fw, j), k, m - 4], (np_, nm)[m - 4]
        return remote(
            src, got.at[turn(got, j), m, k],
            ss[m // 4].at[turn(ss[m // 4], j)], rs[m // 2 > 0].at[turn(rs[m // 2 > 0], j)], to,
        )

    def messages(phase, j, lo, hi):
        got, _, ss, rs = bufs[phase]
        block = got.at[turn(got, j), pl.ds(lo, hi - lo)]
        return remote(block, block, ss[lo // 4].at[turn(ss[lo // 4], j)], rs[lo // 2 > 0].at[turn(rs[lo // 2 > 0], j)], mate)

    def rs_raw(phase, j):
        for m in range(4):
            for k in range(2):
                message(phase, j, k, m).start()

    def rs_forward(phase, j):
        got, fw, _, _ = bufs[phase]
        messages(phase, j, 0, 2).wait_recv()
        for hf in range(2):
            for k in range(2):
                q, _, _ = ring[phase][k]
                qq = q + 1 if hf == 0 else q - 1
                total = term(phase, j, k, qq, hf, True)[...] + got[turn(got, j), hf, k].astype(F32)
                fw[turn(fw, j), k, hf] = total.astype(BF16)
                message(phase, j, k, 4 + hf).start()
        messages(phase, j, 0, 4).wait_send()

    def rs_finish(phase, j, store):
        got, _, _, _ = bufs[phase]
        messages(phase, j, 2, 6).wait_recv()
        for k in range(2):
            q, _, _ = ring[phase][k]
            for hf in range(2):
                total = (
                    term(phase, j, k, q, hf, True)[...]
                    + got[turn(got, j), 4 + hf, k].astype(F32)
                    + got[turn(got, j), 3 - hf, k].astype(F32)
                )
                store(k, hf, total)
        messages(phase, j, 4, 6).wait_send()

    def store_t(j):
        def store(k, hf, total):
            t32[turn(t32, j), k, :, pl.ds(hf * CH, CH)] = total
            t16[turn(t16, j), k, :, pl.ds(hf * CH, CH)] = total.astype(BF16)

        return store

    def y_block(phase, j, k, q, hf=None):
        q1 = ring[1][k][0]
        col = core * C + k * CB + (0 if hf is None else hf * CH)
        cols = pl.ds(pl.multiple_of(col, CH), CB if hf is None else CH)
        if phase == 2:
            row = j * R + q1 * R1 + lax.rem(q + side, side) * R2
            return y.at[pl.ds(pl.multiple_of(row, R2), R2), cols]
        row = j * R + lax.rem(q + side, side) * R1
        return y.at[pl.ds(pl.multiple_of(row, R1), R1), cols]

    gsem = {1: ((sg1a, sg1b), (rg1a, rg1b)), 2: ((sg2a, sg2b), (rg2a, rg2b))}

    def gather(phase, j, k, m):
        ss, rs = (sems[m // 2] for sems in gsem[phase])
        q, np_, nm = ring[phase][k]
        dq, hf = ((0, None), (0, None), (-1, 0), (1, 1))[m]
        block = y_block(phase, j, k, q + dq, hf)
        return remote(block, block, ss.at[turn(ss, j)], rs.at[turn(rs, j)], (np_, nm)[m % 2])

    def gathers(phase, j, late):
        ss, rs = (sems[late] for sems in gsem[phase])
        size = (R1, R)[phase == 1] // (1 + late)
        block = y.at[pl.ds(pl.multiple_of(j * R, R), size), pl.ds(0, CB)]
        return remote(block, block, ss.at[turn(ss, j)], rs.at[turn(rs, j)], mate)

    def ag_start(phase, j):
        for m in range(2):
            for k in range(2):
                gather(phase, j, k, m).start()

    def ag_pass(phase, j):
        gathers(phase, j, 0).wait_recv()
        for m in range(2):
            for k in range(2):
                gather(phase, j, k, 2 + m).start()
        gathers(phase, j, 0).wait_send()

    def ag_end(phase, j):
        gathers(phase, j, 1).wait_recv()
        gathers(phase, j, 1).wait_send()

    def swap(j, k, dq):
        block = y_block(1, j, k, ring[1][k][0] + dq)
        return remote(block, block, sd.at[turn(sd, j)], rd.at[turn(rd, j)], mate)

    def swaps(j):
        block = y.at[pl.ds(pl.multiple_of(j * R, R), R), mate_cols]
        return remote(block, block, sd.at[turn(sd, j)], rd.at[turn(rd, j)], mate)

    def stage2(j):
        rs_finish(1, j, store_t(j))
        rs_raw(2, j)

    def stage4(j):
        def store(k, hf, total):
            q2 = ring[2][k][0]
            y_block(2, j, k, q2, hf)[...] = total.astype(BF16)

        rs_finish(2, j, store)
        ag_start(2, j)

    def stage6(j):
        ag_end(2, j)
        ag_start(1, j)

    def stage7(j):
        ag_pass(1, j)
        for dq in (-1, 0, 1):
            for k in range(2):
                swap(j, k, dq).start()

    def stage8(j):
        ag_end(1, j)
        for k in range(2):
            swap(j, k, 2).start()

    def stage9(j):
        swaps(j).wait_send()
        swaps(j).wait_recv()

    stages = (
        None,
        functools.partial(rs_forward, 1),
        stage2,
        functools.partial(rs_forward, 2),
        stage4,
        functools.partial(ag_pass, 2),
        stage6,
        stage7,
        stage8,
        stage9,
    )

    gate_up_first()

    def step(s, carry):
        def run(i):
            j = s - LAGS[i]

            @pl.when(jnp.logical_and(j >= 0, j < nc))
            def _():
                stages[i](j)

        for i in range(len(stages) - 1, 1, -1):
            run(i)

        @pl.when(s + 1 < nc)
        def _():
            gate_up(s + 1)

        run(1)

        @pl.when(s < nc)
        def _():
            @pl.when(s == 0)
            def _():
                wd_own.wait()
                wd_mate.wait()

            down(s)
            rs_raw(1, s)

        return carry

    lax.fori_loop(0, nc + LAGS[-1], step, 0)


def _store(y, out, sems):
    size = y.shape[0] // STORES
    copies = [
        pltpu.make_async_copy(y.at[pl.ds(i * size, size), :], out.at[pl.ds(i * size, size), :], sems.at[i])
        for i in range(STORES)
    ]
    for copy in copies:
        copy.start()
    for copy in copies:
        copy.wait()


def _mlp(side, x, w_gate, w_up, w_down):
    rows, depth = x.shape
    ff = w_gate.shape[1]
    width = w_down.shape[1]
    C = width // 2
    R = ROWS
    nc = rows // R
    CB, CH = C // 2, C // 4
    R1, R2 = R // side, R // side // side
    L = LAGS
    dma = pltpu.SemaphoreType.DMA
    y = pl.pallas_call(
        functools.partial(_kernel, side, nc),
        out_shape=pltpu.VMEM((rows, width), BF16),
        in_specs=[pl.BlockSpec(memory_space=pl.ANY)] * 4,
        out_specs=pl.BlockSpec(memory_space=pltpu.VMEM),
        scratch_shapes=[
            pltpu.VMEM((2, depth, ff), BF16),
            pltpu.VMEM((2 * ff, C), BF16),
            pltpu.VMEM((2, R, depth), BF16),
            pltpu.VMEM((4, R, 2 * ff), BF16),
            pltpu.VMEM((L[2], R, C), F32),
            pltpu.VMEM((L[1], R, C), BF16),
            pltpu.VMEM((2 * L[2] - L[1], 6, 2, R1, CH), BF16),
            pltpu.VMEM((2 * L[4] - L[3] - L[2], 6, 2, R2, CH), BF16),
            pltpu.VMEM((L[2] - L[1], 2, 2, R1, CH), BF16),
            pltpu.VMEM((L[4] - L[3], 2, 2, R2, CH), BF16),
            pltpu.VMEM((L[4] - L[2], 2, R1, CB), F32),
            pltpu.VMEM((L[3] - L[2], 2, R1, CB), BF16),
            dma((L[1],)), dma((L[2] - L[1],)), dma((L[2],)), dma((2 * L[2] - L[1],)),
            dma((L[3] - L[2],)), dma((L[4] - L[3],)), dma((L[4] - L[2],)), dma((2 * L[4] - L[3] - L[2],)),
            dma((L[5] - L[4],)), dma((L[6] - L[5],)), dma((L[6] - L[4],)), dma((L[6] - L[5] + 2,)),
            dma((L[7] - L[6],)), dma((L[8] - L[7],)), dma((L[8] - L[6],)), dma((L[8] - L[6],)),
            dma((L[9] - L[7],)), dma((L[9] - L[7] + 2,)),
            dma((2,)), dma((4,)),
            dma, dma,
            dma((2,)), dma((AHEAD,)), dma,
        ],
        compiler_params=pltpu.CompilerParams(
            collective_id=0, has_side_effects=True, vmem_limit_bytes=43 * 1024 * 1024,
        ),
        cost_estimate=pl.CostEstimate(
            flops=6 * rows * depth * ff, bytes_accessed=4 * rows * depth, transcendentals=rows * ff,
        ),
    )(x, w_gate, w_up, w_down)
    return pl.pallas_call(
        _store,
        out_shape=jax.ShapeDtypeStruct((rows, width), BF16),
        in_specs=[pl.BlockSpec(memory_space=pl.ANY)],
        out_specs=pl.BlockSpec(memory_space=pl.ANY),
        scratch_shapes=[dma((STORES,))],
        compiler_params=pltpu.CompilerParams(vmem_limit_bytes=1024 * 1024),
        cost_estimate=pl.CostEstimate(flops=0, bytes_accessed=2 * rows * width, transcendentals=0),
    )(pltpu.with_memory_space_constraint(y, pltpu.VMEM))


def solution(mesh):
    side = math.isqrt(mesh.shape["tp"] // 2)

    return jax.shard_map(
        functools.partial(_mlp, side),
        mesh=mesh,
        in_specs=(P("dp", None), P(None, "tp"), P(None, "tp"), P("tp", None)),
        out_specs=P("dp", None),
        check_vma=False,
    )
```

```python
import functools
import math

import jax
import jax.numpy as jnp
from jax import lax
from jax.experimental import pallas as pl
from jax.experimental.pallas import tpu as pltpu
from jax.sharding import PartitionSpec as P

MESH = pl.DeviceIdType.MESH
ROWS = 128
STORES = 8
AHEAD = 3
STAGGER = 4
GAP = 250
KSLICES = 10
LAGS = (0, 2, 4, 6, 8, 10, 14, 19, 25)
F32, BF16 = jnp.float32, jnp.bfloat16


def _kernel(
    side, nc, x_hbm, wg_hbm, wu_hbm, wd_hbm, y,
    w, wd, xb, h, p32, p16, got1, got2, fw1, fw2, t32, t16,
    s1a, s1b, r1a, r1b, s2a, s2b, r2a, r2b, sy, rg2a, rg2b, rg1a, rg1b, rd, sh, rh, swd, rwd, lx, lw, lwd,
):
    R = xb.shape[1]
    K = xb.shape[2]
    FF = w.shape[2]
    C = p32.shape[2]
    CB, CH = C // 2, C // 4
    R1, R2 = R // side, R // side // side

    me = lax.axis_index("tp")
    core = lax.rem(me, 2)
    chip = lax.div(me, 2)
    cx, cy = lax.div(chip, side), lax.rem(chip, side)
    mate = me + 1 - 2 * core

    def dev(a, b):
        return (lax.rem(a + side, side) * side + lax.rem(b + side, side)) * 2 + core

    xp, xm, yp, ym = dev(cx + 1, cy), dev(cx - 1, cy), dev(cx, cy + 1), dev(cx, cy - 1)
    ring = {
        1: ((cx, xp, xm), (cy, yp, ym)),
        2: ((cy, yp, ym), (cx, xp, xm)),
    }

    def remote(src, dst, ssem, rsem, to):
        return pltpu.make_async_remote_copy(
            src_ref=src, dst_ref=dst, send_sem=ssem, recv_sem=rsem,
            device_id={"tp": to}, device_id_type=MESH,
        )

    def turn(ref, j):
        return lax.rem(j, ref.shape[0])

    def load_x(j):
        rows = pl.ds(pl.multiple_of(j * R, R), R)
        slot = lax.rem(j, 2)
        return pltpu.make_async_copy(x_hbm.at[rows, :], xb.at[slot], lx.at[slot])

    KS = K // KSLICES

    def load_w(i):
        rows = pl.ds(i * KS, KS)
        return (
            pltpu.make_async_copy(wg_hbm.at[rows, :], w.at[0, rows, :], lw.at[i % (AHEAD + STAGGER)]),
            pltpu.make_async_copy(wu_hbm.at[rows, :], w.at[1, rows, :], lw.at[i % (AHEAD + STAGGER)]),
        )

    my_cols = pl.ds(pl.multiple_of(core * C, C), C)
    mate_cols = pl.ds(pl.multiple_of((1 - core) * C, C), C)

    barrier = pltpu.get_barrier_semaphore()
    for d in (mate, xp, xm, yp, ym):
        pl.semaphore_signal(barrier, inc=1, device_id={"tp": d}, device_id_type=MESH)
    load_x(0).start()
    for i in range(AHEAD):
        for copy in load_w(i):
            copy.start()
    wd_own = pltpu.make_async_copy(wd_hbm.at[:, my_cols], wd.at[pl.ds(0, FF), :], lwd)

    for i in range(AHEAD, AHEAD + STAGGER):
        pl.delay(GAP)
        for copy in load_w(i):
            copy.start()
    pl.semaphore_wait(barrier, 5)

    wd_mate = remote(wd_hbm.at[:, mate_cols], wd.at[pl.ds(FF, FF), :], swd, rwd, mate)
    wd_mate.start()
    def send_h(j):
        return remote(
            h.at[turn(h, j), :, pl.ds(0, FF)], h.at[turn(h, j), :, pl.ds(FF, FF)],
            sh.at[turn(sh, j)], rh.at[turn(rh, j)], mate,
        )

    TN = min(256, FF)

    def gate_up(j):
        slot = lax.rem(j, 2)
        load_x(j).wait()
        for t in range(FF // TN):
            cols = pl.ds(t * TN, TN)
            g = jnp.dot(xb[slot], w[0, :, cols], preferred_element_type=F32)
            u = jnp.dot(xb[slot], w[1, :, cols], preferred_element_type=F32)
            h[turn(h, j), :, cols] = (jax.nn.silu(g) * u).astype(BF16)
        send_h(j).start()

        @pl.when(j + 2 < nc)
        def _():
            load_x(j + 2).start()

    def gate_up_first():
        load_x(0).wait()
        for i in range(KSLICES):
            part = pl.ds(i * KS, KS)
            pltpu.make_async_copy(w.at[:, part, :], w.at[:, part, :], lw.at[i % (AHEAD + STAGGER)]).wait()
            if i + AHEAD + STAGGER < KSLICES:
                for copy in load_w(i + AHEAD + STAGGER):
                    copy.start()
            elif i + AHEAD + STAGGER == KSLICES:
                load_x(1).start()
                wd_own.start()
            g = jnp.dot(xb[0, :, part], w[0, part, :], preferred_element_type=F32)
            u = jnp.dot(xb[0, :, part], w[1, part, :], preferred_element_type=F32)
            if i > 0:
                g, u = p32[0, :, pl.ds(0, FF)] + g, p32[1, :, pl.ds(0, FF)] + u
            if i < KSLICES - 1:
                p32[0, :, pl.ds(0, FF)] = g
                p32[1, :, pl.ds(0, FF)] = u
            else:
                h[0, :, pl.ds(0, FF)] = (jax.nn.silu(g) * u).astype(BF16)
        send_h(0).start()
        load_x(2).start()

    TD = 512 if C % 512 == 0 else CH

    def down(j):
        send_h(j).wait()
        for t in range(C // TD):
            cols = pl.ds(t * TD, TD)
            p = jnp.dot(h[turn(h, j)], wd[:, cols], preferred_element_type=F32)
            p32[turn(p32, j), :, cols] = p
            p16[turn(p16, j), :, cols] = p.astype(BF16)

    def piece(phase, q):
        size = R1 if phase == 1 else R2
        return pl.ds(pl.multiple_of(lax.rem(q + side, side) * size, size), size)

    def half(phase, k, hf):
        return pl.ds((k * CB if phase == 1 else 0) + hf * CH, CH)

    def term(phase, j, k, q, hf, wide):
        where = (piece(phase, q), half(phase, k, hf))
        if phase == 1:
            ref = p32 if wide else p16
            return ref.at[turn(ref, j), *where]
        ref = t32 if wide else t16
        return ref.at[turn(ref, j), k, *where]

    bufs = {1: (got1, fw1, (s1a, s1b), (r1a, r1b)), 2: (got2, fw2, (s2a, s2b), (r2a, r2b))}

    def message(phase, j, k, m):
        got, fw, ss, rs = bufs[phase]
        q, np_, nm = ring[phase][k]
        if m < 4:
            dq, hf, to = ((2, 0, np_), (2, 1, nm), (1, 1, np_), (-1, 0, nm))[m]
            src = term(phase, j, k, q + dq, hf, False)
        else:
            src, to = fw.at[turn(fw, j), k, m - 4], (np_, nm)[m - 4]
        return remote(
            src, got.at[turn(got, j), m, k],
            ss[m // 4].at[turn(ss[m // 4], j)], rs[m // 2 > 0].at[turn(rs[m // 2 > 0], j)], to,
        )

    def messages(phase, j, lo, hi):
        got, _, ss, rs = bufs[phase]
        block = got.at[turn(got, j), pl.ds(lo, hi - lo)]
        return remote(block, block, ss[lo // 4].at[turn(ss[lo // 4], j)], rs[lo // 2 > 0].at[turn(rs[lo // 2 > 0], j)], mate)

    def rs_raw(phase, j):
        for m in range(4):
            for k in range(2):
                message(phase, j, k, m).start()

    def rs_forward(phase, j):
        got, fw, _, _ = bufs[phase]
        messages(phase, j, 0, 2).wait_recv()
        for hf in range(2):
            for k in range(2):
                q, _, _ = ring[phase][k]
                qq = q + 1 if hf == 0 else q - 1
                total = term(phase, j, k, qq, hf, True)[...] + got[turn(got, j), hf, k].astype(F32)
                fw[turn(fw, j), k, hf] = total.astype(BF16)
                message(phase, j, k, 4 + hf).start()
        messages(phase, j, 0, 4).wait_send()

    def rs_finish(phase, j, store):
        got, _, _, _ = bufs[phase]
        messages(phase, j, 2, 6).wait_recv()
        for k in range(2):
            q, _, _ = ring[phase][k]
            for hf in range(2):
                total = (
                    term(phase, j, k, q, hf, True)[...]
                    + got[turn(got, j), 4 + hf, k].astype(F32)
                    + got[turn(got, j), 3 - hf, k].astype(F32)
                )
                store(k, hf, total)
        messages(phase, j, 4, 6).wait_send()

    def store_t(j):
        def store(k, hf, total):
            t32[turn(t32, j), k, :, pl.ds(hf * CH, CH)] = total
            t16[turn(t16, j), k, :, pl.ds(hf * CH, CH)] = total.astype(BF16)

        return store

    def y_block(phase, j, k, q, hf=None):
        q1 = ring[1][k][0]
        col = core * C + k * CB + (0 if hf is None else hf * CH)
        cols = pl.ds(pl.multiple_of(col, CH), CB if hf is None else CH)
        if phase == 2:
            row = j * R + q1 * R1 + lax.rem(q + side, side) * R2
            return y.at[pl.ds(pl.multiple_of(row, R2), R2), cols]
        row = j * R + lax.rem(q + side, side) * R1
        return y.at[pl.ds(pl.multiple_of(row, R1), R1), cols]

    gsem = {1: (rg1a, rg1b), 2: (rg2a, rg2b)}

    def gather(phase, j, k, m):
        rs = gsem[phase][m // 2]
        q, np_, nm = ring[phase][k]
        dq, hf = ((0, None), (0, None), (-1, 0), (1, 1))[m]
        block = y_block(phase, j, k, q + dq, hf)
        return remote(block, block, sy, rs.at[turn(rs, j)], (np_, nm)[m % 2])

    def gathers(phase, j, late):
        rs = gsem[phase][late]
        size = (R1, R)[phase == 1] // (1 + late)
        block = y.at[pl.ds(pl.multiple_of(j * R, R), size), pl.ds(0, CB)]
        return remote(block, block, sy, rs.at[turn(rs, j)], mate)

    def ag_start(phase, j):
        for m in range(2):
            for k in range(2):
                gather(phase, j, k, m).start()

    def ag_pass(phase, j):
        gathers(phase, j, 0).wait_recv()
        for m in range(2):
            for k in range(2):
                gather(phase, j, k, 2 + m).start()

    def ag_end(phase, j):
        gathers(phase, j, 1).wait_recv()

    def swap(j, k, dq):
        block = y_block(1, j, k, ring[1][k][0] + dq)
        return remote(block, block, sy, rd, mate)

    def stage2(j):
        rs_finish(1, j, store_t(j))
        rs_raw(2, j)

    def stage4(j):
        def store(k, hf, total):
            q2 = ring[2][k][0]
            y_block(2, j, k, q2, hf)[...] = total.astype(BF16)

        rs_finish(2, j, store)
        ag_start(2, j)

    def stage6(j):
        ag_end(2, j)
        ag_start(1, j)

    def stage7(j):
        ag_pass(1, j)
        for dq in (-1, 0, 1):
            for k in range(2):
                swap(j, k, dq).start()

    def stage8(j):
        ag_end(1, j)
        for k in range(2):
            swap(j, k, 2).start()

    stages = (
        None,
        functools.partial(rs_forward, 1),
        stage2,
        functools.partial(rs_forward, 2),
        stage4,
        functools.partial(ag_pass, 2),
        stage6,
        stage7,
        stage8,
    )

    gate_up_first()

    def step(s, carry):
        def run(i):
            j = s - LAGS[i]

            @pl.when(jnp.logical_and(j >= 0, j < nc))
            def _():
                stages[i](j)

        for i in range(len(stages) - 1, 1, -1):
            run(i)

        @pl.when(s + 1 < nc)
        def _():
            gate_up(s + 1)

        run(1)

        @pl.when(s < nc)
        def _():
            @pl.when(s == 0)
            def _():
                wd_own.wait()
                wd_mate.wait()

            down(s)
            rs_raw(1, s)

        return carry

    lax.fori_loop(0, nc + LAGS[-1], step, 0)

    half_y = y.at[:, mate_cols]
    remote(half_y, half_y, sy, rd, mate).wait_recv()
    sent = y.at[pl.ds(0, nc * (R + 3 * (R1 + R2)) // 2), :]
    remote(sent, sent, sy, rd, mate).wait_send()


def _store(y, out, sems):
    size = y.shape[0] // STORES
    copies = [
        pltpu.make_async_copy(y.at[pl.ds(i * size, size), :], out.at[pl.ds(i * size, size), :], sems.at[i])
        for i in range(STORES)
    ]
    for copy in copies:
        copy.start()
    for copy in copies:
        copy.wait()


def _mlp(side, x, w_gate, w_up, w_down):
    rows, depth = x.shape
    ff = w_gate.shape[1]
    width = w_down.shape[1]
    C = width // 2
    R = ROWS
    nc = rows // R
    CB, CH = C // 2, C // 4
    R1, R2 = R // side, R // side // side
    L = LAGS
    dma = pltpu.SemaphoreType.DMA
    y = pl.pallas_call(
        functools.partial(_kernel, side, nc),
        out_shape=pltpu.VMEM((rows, width), BF16),
        in_specs=[pl.BlockSpec(memory_space=pl.ANY)] * 4,
        out_specs=pl.BlockSpec(memory_space=pltpu.VMEM),
        scratch_shapes=[
            pltpu.VMEM((2, depth, ff), BF16),
            pltpu.VMEM((2 * ff, C), BF16),
            pltpu.VMEM((2, R, depth), BF16),
            pltpu.VMEM((4, R, 2 * ff), BF16),
            pltpu.VMEM((L[2], R, C), F32),
            pltpu.VMEM((L[1], R, C), BF16),
            pltpu.VMEM((2 * L[2] - L[1], 6, 2, R1, CH), BF16),
            pltpu.VMEM((2 * L[4] - L[3] - L[2], 6, 2, R2, CH), BF16),
            pltpu.VMEM((L[2] - L[1], 2, 2, R1, CH), BF16),
            pltpu.VMEM((L[4] - L[3], 2, 2, R2, CH), BF16),
            pltpu.VMEM((L[4] - L[2], 2, R1, CB), F32),
            pltpu.VMEM((L[3] - L[2], 2, R1, CB), BF16),
            dma((L[1],)), dma((L[2] - L[1],)), dma((L[2],)), dma((2 * L[2] - L[1],)),
            dma((L[3] - L[2],)), dma((L[4] - L[3],)), dma((L[4] - L[2],)), dma((2 * L[4] - L[3] - L[2],)),
            dma, dma((L[6] - L[4],)), dma((L[6] - L[5] + 2,)), dma((L[8] - L[6],)), dma((L[8] - L[6],)), dma,
            dma((2,)), dma((4,)),
            dma, dma,
            dma((2,)), dma((AHEAD + STAGGER,)), dma,
        ],
        compiler_params=pltpu.CompilerParams(
            collective_id=0, has_side_effects=True, vmem_limit_bytes=43 * 1024 * 1024,
        ),
        cost_estimate=pl.CostEstimate(
            flops=6 * rows * depth * ff, bytes_accessed=4 * rows * depth, transcendentals=rows * ff,
        ),
    )(x, w_gate, w_up, w_down)
    return pl.pallas_call(
        _store,
        out_shape=jax.ShapeDtypeStruct((rows, width), BF16),
        in_specs=[pl.BlockSpec(memory_space=pl.ANY)],
        out_specs=pl.BlockSpec(memory_space=pl.ANY),
        scratch_shapes=[dma((STORES,))],
        compiler_params=pltpu.CompilerParams(vmem_limit_bytes=1024 * 1024),
        cost_estimate=pl.CostEstimate(flops=0, bytes_accessed=2 * rows * width, transcendentals=0),
    )(pltpu.with_memory_space_constraint(y, pltpu.VMEM))


def solution(mesh):
    side = math.isqrt(mesh.shape["tp"] // 2)

    return jax.shard_map(
        functools.partial(_mlp, side),
        mesh=mesh,
        in_specs=(P("dp", None), P(None, "tp"), P(None, "tp"), P("tp", None)),
        out_specs=P("dp", None),
        check_vma=False,
    )
```

```python
import functools
import math

import jax
import jax.numpy as jnp
from jax import lax
from jax.experimental import pallas as pl
from jax.experimental.pallas import tpu as pltpu
from jax.sharding import PartitionSpec as P

MESH = pl.DeviceIdType.MESH
ROWS = 128
STORES = 8
AHEAD = 3
STAGGER = 4
GAP = 250
KSLICES = 10
LAGS = (0, 2, 4, 6, 8, 10, 15, 20, 26)
F32, BF16 = jnp.float32, jnp.bfloat16


def _kernel(
    side, nc, x_hbm, wg_hbm, wu_hbm, wd_hbm, y,
    w, wd, xb, h, p32, p16, got1, got2, fw1, fw2, t32, t16,
    s1a, s1b, r1a, r1b, s2a, s2b, r2a, r2b, sy, rg2a, rg2b, rg1a, rg1b, rd, sh, rh, swd, rwd, lx, lwd,
):
    R = xb.shape[1]
    K = xb.shape[2]
    FF = w.shape[2]
    C = p32.shape[2]
    CB, CH = C // 2, C // 4
    R1, R2 = R // side, R // side // side

    me = lax.axis_index("tp")
    core = lax.rem(me, 2)
    chip = lax.div(me, 2)
    cx, cy = lax.div(chip, side), lax.rem(chip, side)
    mate = me + 1 - 2 * core

    def dev(a, b):
        return (lax.rem(a + side, side) * side + lax.rem(b + side, side)) * 2 + core

    xp, xm, yp, ym = dev(cx + 1, cy), dev(cx - 1, cy), dev(cx, cy + 1), dev(cx, cy - 1)
    ring = {
        1: ((cx, xp, xm), (cy, yp, ym)),
        2: ((cy, yp, ym), (cx, xp, xm)),
    }

    def remote(src, dst, ssem, rsem, to):
        return pltpu.make_async_remote_copy(
            src_ref=src, dst_ref=dst, send_sem=ssem, recv_sem=rsem,
            device_id={"tp": to}, device_id_type=MESH,
        )

    def turn(ref, j):
        return lax.rem(j, ref.shape[0])

    def load_x(j):
        rows = pl.ds(pl.multiple_of(j * R, R), R)
        slot = lax.rem(j, 2)
        return pltpu.make_async_copy(x_hbm.at[rows, :], xb.at[slot], lx.at[slot])

    KS = K // KSLICES

    def load_w(i):
        rows = pl.ds(i * KS, KS)
        return (
            pltpu.make_async_copy(wg_hbm.at[rows, :], w.at[0, rows, :], rg1b.at[i % (AHEAD + STAGGER)]),
            pltpu.make_async_copy(wu_hbm.at[rows, :], w.at[1, rows, :], rg1b.at[i % (AHEAD + STAGGER)]),
        )

    my_cols = pl.ds(pl.multiple_of(core * C, C), C)
    mate_cols = pl.ds(pl.multiple_of((1 - core) * C, C), C)

    barrier = pltpu.get_barrier_semaphore()
    for d in (mate, xp, xm, yp, ym):
        pl.semaphore_signal(barrier, inc=1, device_id={"tp": d}, device_id_type=MESH)
    load_x(0).start()
    for i in range(AHEAD):
        for copy in load_w(i):
            copy.start()
    wd_own = pltpu.make_async_copy(wd_hbm.at[:, my_cols], wd.at[pl.ds(0, FF), :], lwd)

    for i in range(AHEAD, AHEAD + STAGGER):
        pl.delay(GAP)
        for copy in load_w(i):
            copy.start()
    pl.semaphore_wait(barrier, 5)

    wd_mate = remote(wd_hbm.at[:, mate_cols], wd.at[pl.ds(FF, FF), :], swd, rwd, mate)
    wd_mate.start()
    def send_h(j):
        return remote(
            h.at[turn(h, j), :, pl.ds(0, FF)], h.at[turn(h, j), :, pl.ds(FF, FF)],
            sh.at[turn(sh, j)], rh.at[turn(rh, j)], mate,
        )

    TN = min(256, FF)

    def gate_up(j):
        slot = lax.rem(j, 2)
        load_x(j).wait()
        for t in range(FF // TN):
            cols = pl.ds(t * TN, TN)
            g = jnp.dot(xb[slot], w[0, :, cols], preferred_element_type=F32)
            u = jnp.dot(xb[slot], w[1, :, cols], preferred_element_type=F32)
            h[turn(h, j), :, cols] = (jax.nn.silu(g) * u).astype(BF16)
        send_h(j).start()

        @pl.when(j + 2 < nc)
        def _():
            load_x(j + 2).start()

    def gate_up_first():
        load_x(0).wait()
        for i in range(KSLICES):
            part = pl.ds(i * KS, KS)
            pltpu.make_async_copy(w.at[:, part, :], w.at[:, part, :], rg1b.at[i % (AHEAD + STAGGER)]).wait()
            if i + AHEAD + STAGGER < KSLICES:
                for copy in load_w(i + AHEAD + STAGGER):
                    copy.start()
            elif i + AHEAD + STAGGER == KSLICES:
                load_x(1).start()
            if i == 8:
                wd_own.start()
            g = jnp.dot(xb[0, :, part], w[0, part, :], preferred_element_type=F32)
            u = jnp.dot(xb[0, :, part], w[1, part, :], preferred_element_type=F32)
            if i > 0:
                g, u = p32[0, :, pl.ds(0, FF)] + g, p32[1, :, pl.ds(0, FF)] + u
            if i < KSLICES - 1:
                p32[0, :, pl.ds(0, FF)] = g
                p32[1, :, pl.ds(0, FF)] = u
            else:
                h[0, :, pl.ds(0, FF)] = (jax.nn.silu(g) * u).astype(BF16)
        send_h(0).start()
        load_x(2).start()

    TD = 512 if C % 512 == 0 else CH

    def down(j):
        send_h(j).wait()
        for t in range(C // TD):
            cols = pl.ds(t * TD, TD)
            p = jnp.dot(h[turn(h, j)], wd[:, cols], preferred_element_type=F32)
            p32[turn(p32, j), :, cols] = p
            p16[turn(p16, j), :, cols] = p.astype(BF16)

    def piece(phase, q):
        size = R1 if phase == 1 else R2
        return pl.ds(pl.multiple_of(lax.rem(q + side, side) * size, size), size)

    def half(phase, k, hf):
        return pl.ds((k * CB if phase == 1 else 0) + hf * CH, CH)

    def term(phase, j, k, q, hf, wide):
        where = (piece(phase, q), half(phase, k, hf))
        if phase == 1:
            ref = p32 if wide else p16
            return ref.at[turn(ref, j), *where]
        ref = t32 if wide else t16
        return ref.at[turn(ref, j), k, *where]

    bufs = {1: (got1, fw1, (s1a, s1b), (r1a, r1b)), 2: (got2, fw2, (s2a, s2b), (r2a, r2b))}

    def message(phase, j, k, m):
        got, fw, ss, rs = bufs[phase]
        q, np_, nm = ring[phase][k]
        if m < 4:
            dq, hf, to = ((2, 0, np_), (2, 1, nm), (1, 1, np_), (-1, 0, nm))[m]
            src = term(phase, j, k, q + dq, hf, False)
        else:
            src, to = fw.at[turn(fw, j), k, m - 4], (np_, nm)[m - 4]
        return remote(
            src, got.at[turn(got, j), m, k],
            ss[m // 4].at[turn(ss[m // 4], j)], rs[m // 2 > 0].at[turn(rs[m // 2 > 0], j)], to,
        )

    def messages(phase, j, lo, hi):
        got, _, ss, rs = bufs[phase]
        block = got.at[turn(got, j), pl.ds(lo, hi - lo)]
        return remote(block, block, ss[lo // 4].at[turn(ss[lo // 4], j)], rs[lo // 2 > 0].at[turn(rs[lo // 2 > 0], j)], mate)

    def rs_raw(phase, j):
        for m in range(4):
            for k in range(2):
                message(phase, j, k, m).start()

    def rs_forward(phase, j):
        got, fw, _, _ = bufs[phase]
        messages(phase, j, 0, 2).wait_recv()
        for hf in range(2):
            for k in range(2):
                q, _, _ = ring[phase][k]
                qq = q + 1 if hf == 0 else q - 1
                total = term(phase, j, k, qq, hf, True)[...] + got[turn(got, j), hf, k].astype(F32)
                fw[turn(fw, j), k, hf] = total.astype(BF16)
                message(phase, j, k, 4 + hf).start()
        messages(phase, j, 0, 4).wait_send()

    def rs_finish(phase, j, store):
        got, _, _, _ = bufs[phase]
        messages(phase, j, 2, 6).wait_recv()
        for k in range(2):
            q, _, _ = ring[phase][k]
            for hf in range(2):
                total = (
                    term(phase, j, k, q, hf, True)[...]
                    + got[turn(got, j), 4 + hf, k].astype(F32)
                    + got[turn(got, j), 3 - hf, k].astype(F32)
                )
                store(k, hf, total)
        messages(phase, j, 4, 6).wait_send()

    def store_t(j):
        def store(k, hf, total):
            t32[turn(t32, j), k, :, pl.ds(hf * CH, CH)] = total
            t16[turn(t16, j), k, :, pl.ds(hf * CH, CH)] = total.astype(BF16)

        return store

    def y_block(phase, j, k, q, hf=None):
        q1 = ring[1][k][0]
        col = core * C + k * CB + (0 if hf is None else hf * CH)
        cols = pl.ds(pl.multiple_of(col, CH), CB if hf is None else CH)
        if phase == 2:
            row = j * R + q1 * R1 + lax.rem(q + side, side) * R2
            return y.at[pl.ds(pl.multiple_of(row, R2), R2), cols]
        row = j * R + lax.rem(q + side, side) * R1
        return y.at[pl.ds(pl.multiple_of(row, R1), R1), cols]

    gsem = {1: (rg1a, rg1b), 2: (rg2a, rg2b)}

    def gather(phase, j, k, m):
        rs = gsem[phase][m // 2]
        q, np_, nm = ring[phase][k]
        dq, hf = ((0, None), (0, None), (-1, 0), (1, 1))[m]
        block = y_block(phase, j, k, q + dq, hf)
        return remote(block, block, sy, rs.at[turn(rs, j)], (np_, nm)[m % 2])

    def gathers(phase, j, late):
        rs = gsem[phase][late]
        size = (R1, R)[phase == 1] // (1 + late)
        block = y.at[pl.ds(pl.multiple_of(j * R, R), size), pl.ds(0, CB)]
        return remote(block, block, sy, rs.at[turn(rs, j)], mate)

    def ag_start(phase, j):
        for m in range(2):
            for k in range(2):
                gather(phase, j, k, m).start()

    def ag_pass(phase, j):
        gathers(phase, j, 0).wait_recv()
        for m in range(2):
            for k in range(2):
                gather(phase, j, k, 2 + m).start()

    def ag_end(phase, j):
        gathers(phase, j, 1).wait_recv()

    def swap(j, k, dq):
        block = y_block(1, j, k, ring[1][k][0] + dq)
        return remote(block, block, sy, rd, mate)

    def stage2(j):
        rs_finish(1, j, store_t(j))
        rs_raw(2, j)

    def stage4(j):
        def store(k, hf, total):
            q2 = ring[2][k][0]
            y_block(2, j, k, q2, hf)[...] = total.astype(BF16)

        rs_finish(2, j, store)
        ag_start(2, j)

    def stage6(j):
        ag_end(2, j)
        ag_start(1, j)

    def stage7(j):
        ag_pass(1, j)
        for dq in (-1, 0, 1):
            for k in range(2):
                swap(j, k, dq).start()

    def stage8(j):
        ag_end(1, j)
        for k in range(2):
            swap(j, k, 2).start()

    stages = (
        None,
        functools.partial(rs_forward, 1),
        stage2,
        functools.partial(rs_forward, 2),
        stage4,
        functools.partial(ag_pass, 2),
        stage6,
        stage7,
        stage8,
    )

    gate_up_first()

    def step(s, carry):
        def run(i):
            j = s - LAGS[i]

            @pl.when(jnp.logical_and(j >= 0, j < nc))
            def _():
                stages[i](j)

        for i in range(len(stages) - 1, 1, -1):
            run(i)

        @pl.when(s + 1 < nc)
        def _():
            gate_up(s + 1)

        run(1)

        @pl.when(s < nc)
        def _():
            @pl.when(s == 0)
            def _():
                wd_own.wait()
                wd_mate.wait()

            down(s)
            rs_raw(1, s)

        return carry

    lax.fori_loop(0, nc + LAGS[-1], step, 0)

    half_y = y.at[:, mate_cols]
    remote(half_y, half_y, sy, rd, mate).wait_recv()
    sent = y.at[pl.ds(0, nc * (R + 3 * (R1 + R2)) // 2), :]
    remote(sent, sent, sy, rd, mate).wait_send()


def _store(y, out, sems):
    size = y.shape[0] // STORES
    copies = [
        pltpu.make_async_copy(y.at[pl.ds(i * size, size), :], out.at[pl.ds(i * size, size), :], sems.at[i])
        for i in range(STORES)
    ]
    for copy in copies:
        copy.start()
    for copy in copies:
        copy.wait()


def _mlp(side, x, w_gate, w_up, w_down):
    rows, depth = x.shape
    ff = w_gate.shape[1]
    width = w_down.shape[1]
    C = width // 2
    R = ROWS
    nc = rows // R
    CB, CH = C // 2, C // 4
    R1, R2 = R // side, R // side // side
    L = LAGS
    dma = pltpu.SemaphoreType.DMA
    y = pl.pallas_call(
        functools.partial(_kernel, side, nc),
        out_shape=pltpu.VMEM((rows, width), BF16),
        in_specs=[pl.BlockSpec(memory_space=pl.ANY)] * 4,
        out_specs=pl.BlockSpec(memory_space=pltpu.VMEM),
        scratch_shapes=[
            pltpu.VMEM((2, depth, ff), BF16),
            pltpu.VMEM((2 * ff, C), BF16),
            pltpu.VMEM((2, R, depth), BF16),
            pltpu.VMEM((4, R, 2 * ff), BF16),
            pltpu.VMEM((L[2], R, C), F32),
            pltpu.VMEM((L[1], R, C), BF16),
            pltpu.VMEM((2 * L[2] - L[1], 6, 2, R1, CH), BF16),
            pltpu.VMEM((2 * L[4] - L[3] - L[2], 6, 2, R2, CH), BF16),
            pltpu.VMEM((L[2] - L[1], 2, 2, R1, CH), BF16),
            pltpu.VMEM((L[4] - L[3], 2, 2, R2, CH), BF16),
            pltpu.VMEM((L[4] - L[2], 2, R1, CB), F32),
            pltpu.VMEM((L[3] - L[2], 2, R1, CB), BF16),
            dma((L[1],)), dma((L[2] - L[1],)), dma((L[2],)), dma((2 * L[2] - L[1],)),
            dma((L[3] - L[2],)), dma((L[4] - L[3],)), dma((L[4] - L[2],)), dma((2 * L[4] - L[3] - L[2],)),
            dma, dma((L[6] - L[4],)), dma((L[6] - L[5] + 2,)), dma((L[8] - L[6],)), dma((L[8] - L[6],)), dma,
            dma((2,)), dma((4,)),
            dma, dma,
            dma((2,)), dma,
        ],
        compiler_params=pltpu.CompilerParams(
            collective_id=0, has_side_effects=True, vmem_limit_bytes=43 * 1024 * 1024,
        ),
        cost_estimate=pl.CostEstimate(
            flops=6 * rows * depth * ff, bytes_accessed=4 * rows * depth, transcendentals=rows * ff,
        ),
    )(x, w_gate, w_up, w_down)
    return pl.pallas_call(
        _store,
        out_shape=jax.ShapeDtypeStruct((rows, width), BF16),
        in_specs=[pl.BlockSpec(memory_space=pl.ANY)],
        out_specs=pl.BlockSpec(memory_space=pl.ANY),
        scratch_shapes=[dma((STORES,))],
        compiler_params=pltpu.CompilerParams(vmem_limit_bytes=1024 * 1024),
        cost_estimate=pl.CostEstimate(flops=0, bytes_accessed=2 * rows * width, transcendentals=0),
    )(pltpu.with_memory_space_constraint(y, pltpu.VMEM))


def solution(mesh):
    side = math.isqrt(mesh.shape["tp"] // 2)

    return jax.shard_map(
        functools.partial(_mlp, side),
        mesh=mesh,
        in_specs=(P("dp", None), P(None, "tp"), P(None, "tp"), P("tp", None)),
        out_specs=P("dp", None),
        check_vma=False,
    )
```

```python
import functools
import math

import jax
import jax.numpy as jnp
from jax import lax
from jax.experimental import pallas as pl
from jax.experimental.pallas import tpu as pltpu
from jax.sharding import PartitionSpec as P

MESH = pl.DeviceIdType.MESH
ROWS = 128
STORES = 8
AHEAD = 3
STAGGER = 4
GAP = 250
KSLICES = 10
LAGS = (0, 2, 4, 6, 8, 10, 15, 20, 26)
F32, BF16 = jnp.float32, jnp.bfloat16


def _kernel(
    side, nc, x_hbm, wg_hbm, wu_hbm, wd_hbm, y,
    w, wd, xb, h, p32, p16, got1, got2, fw1, fw2, t32, t16,
    s1a, s1b, r1a, r1b, s2a, s2b, r2a, r2b, sy, rg2a, rg2b, rg1a, rg1b, rd, sh, rh, lx,
):
    R = xb.shape[1]
    K = xb.shape[2]
    FF = w.shape[2]
    C = p32.shape[2]
    CB, CH = C // 2, C // 4
    R1, R2 = R // side, R // side // side

    me = lax.axis_index("tp")
    core = lax.rem(me, 2)
    chip = lax.div(me, 2)
    cx, cy = lax.div(chip, side), lax.rem(chip, side)
    mate = me + 1 - 2 * core

    def dev(a, b):
        return (lax.rem(a + side, side) * side + lax.rem(b + side, side)) * 2 + core

    xp, xm, yp, ym = dev(cx + 1, cy), dev(cx - 1, cy), dev(cx, cy + 1), dev(cx, cy - 1)
    ring = {
        1: ((cx, xp, xm), (cy, yp, ym)),
        2: ((cy, yp, ym), (cx, xp, xm)),
    }

    def remote(src, dst, ssem, rsem, to):
        return pltpu.make_async_remote_copy(
            src_ref=src, dst_ref=dst, send_sem=ssem, recv_sem=rsem,
            device_id={"tp": to}, device_id_type=MESH,
        )

    def turn(ref, j):
        return lax.rem(j, ref.shape[0])

    def load_x(j):
        rows = pl.ds(pl.multiple_of(j * R, R), R)
        slot = lax.rem(j, 2)
        return pltpu.make_async_copy(x_hbm.at[rows, :], xb.at[slot], lx.at[slot])

    KS = K // KSLICES

    def load_w(i):
        rows = pl.ds(i * KS, KS)
        return (
            pltpu.make_async_copy(wg_hbm.at[rows, :], w.at[0, rows, :], rg1b.at[i % (AHEAD + STAGGER)]),
            pltpu.make_async_copy(wu_hbm.at[rows, :], w.at[1, rows, :], rg1b.at[i % (AHEAD + STAGGER)]),
        )

    my_cols = pl.ds(pl.multiple_of(core * C, C), C)
    mate_cols = pl.ds(pl.multiple_of((1 - core) * C, C), C)

    barrier = pltpu.get_barrier_semaphore()
    for d in (mate, xp, xm, yp, ym):
        pl.semaphore_signal(barrier, inc=1, device_id={"tp": d}, device_id_type=MESH)
    load_x(0).start()
    for i in range(AHEAD):
        for copy in load_w(i):
            copy.start()
    wd_own = pltpu.make_async_copy(wd_hbm.at[:, my_cols], wd.at[pl.ds(0, FF), :], s2b.at[0])

    for i in range(AHEAD, AHEAD + STAGGER):
        pl.delay(GAP)
        for copy in load_w(i):
            copy.start()
    pl.semaphore_wait(barrier, 5)

    wd_mate = remote(wd_hbm.at[:, mate_cols], wd.at[pl.ds(FF, FF), :], s2a.at[0], r2b.at[0], mate)
    wd_mate.start()
    def send_h(j):
        return remote(
            h.at[turn(h, j), :, pl.ds(0, FF)], h.at[turn(h, j), :, pl.ds(FF, FF)],
            sh.at[turn(sh, j)], rh.at[turn(rh, j)], mate,
        )

    TN = min(512, FF)

    def gate_up(j):
        slot = lax.rem(j, 2)
        load_x(j).wait()
        for t in range(FF // TN):
            cols = pl.ds(t * TN, TN)
            g = jnp.dot(xb[slot], w[0, :, cols], preferred_element_type=F32)
            u = jnp.dot(xb[slot], w[1, :, cols], preferred_element_type=F32)
            h[turn(h, j), :, cols] = (jax.nn.silu(g) * u).astype(BF16)
        send_h(j).start()

        @pl.when(j + 2 < nc)
        def _():
            load_x(j + 2).start()

    def gate_up_first():
        load_x(0).wait()
        for i in range(KSLICES):
            part = pl.ds(i * KS, KS)
            pltpu.make_async_copy(w.at[:, part, :], w.at[:, part, :], rg1b.at[i % (AHEAD + STAGGER)]).wait()
            if i + AHEAD + STAGGER < KSLICES:
                for copy in load_w(i + AHEAD + STAGGER):
                    copy.start()
            elif i + AHEAD + STAGGER == KSLICES:
                load_x(1).start()
            if i == 8:
                wd_own.start()
            g = jnp.dot(xb[0, :, part], w[0, part, :], preferred_element_type=F32)
            u = jnp.dot(xb[0, :, part], w[1, part, :], preferred_element_type=F32)
            if i > 0:
                g, u = p32[0, :, pl.ds(0, FF)] + g, p32[1, :, pl.ds(0, FF)] + u
            if i < KSLICES - 1:
                p32[0, :, pl.ds(0, FF)] = g
                p32[1, :, pl.ds(0, FF)] = u
            else:
                h[0, :, pl.ds(0, FF)] = (jax.nn.silu(g) * u).astype(BF16)
        send_h(0).start()
        load_x(2).start()

    TD = CB

    def down(j):
        send_h(j).wait()
        for t in range(C // TD):
            cols = pl.ds(t * TD, TD)
            p = jnp.dot(h[turn(h, j)], wd[:, cols], preferred_element_type=F32)
            p32[turn(p32, j), :, cols] = p
            p16[turn(p16, j), :, cols] = p.astype(BF16)

    def piece(phase, q):
        size = R1 if phase == 1 else R2
        return pl.ds(pl.multiple_of(lax.rem(q + side, side) * size, size), size)

    def half(phase, k, hf):
        return pl.ds((k * CB if phase == 1 else 0) + hf * CH, CH)

    def term(phase, j, k, q, hf, wide):
        where = (piece(phase, q), half(phase, k, hf))
        if phase == 1:
            ref = p32 if wide else p16
            return ref.at[turn(ref, j), *where]
        ref = t32 if wide else t16
        return ref.at[turn(ref, j), k, *where]

    bufs = {1: (got1, fw1, (s1a, s1b), (r1a, r1b)), 2: (got2, fw2, (s2a, s2b), (r2a, r2b))}

    def message(phase, j, k, m):
        got, fw, ss, rs = bufs[phase]
        q, np_, nm = ring[phase][k]
        if m < 4:
            dq, hf, to = ((2, 0, np_), (2, 1, nm), (1, 1, np_), (-1, 0, nm))[m]
            src = term(phase, j, k, q + dq, hf, False)
        else:
            src, to = fw.at[turn(fw, j), k, m - 4], (np_, nm)[m - 4]
        return remote(
            src, got.at[turn(got, j), m, k],
            ss[m // 4].at[turn(ss[m // 4], j)], rs[m // 2 > 0].at[turn(rs[m // 2 > 0], j)], to,
        )

    def messages(phase, j, lo, hi):
        got, _, ss, rs = bufs[phase]
        block = got.at[turn(got, j), pl.ds(lo, hi - lo)]
        return remote(block, block, ss[lo // 4].at[turn(ss[lo // 4], j)], rs[lo // 2 > 0].at[turn(rs[lo // 2 > 0], j)], mate)

    def rs_raw(phase, j):
        for m in range(4):
            for k in range(2):
                message(phase, j, k, m).start()

    def rs_forward(phase, j):
        got, fw, _, _ = bufs[phase]
        messages(phase, j, 0, 2).wait_recv()
        for hf in range(2):
            for k in range(2):
                q, _, _ = ring[phase][k]
                qq = q + 1 if hf == 0 else q - 1
                total = term(phase, j, k, qq, hf, True)[...] + got[turn(got, j), hf, k].astype(F32)
                fw[turn(fw, j), k, hf] = total.astype(BF16)
                message(phase, j, k, 4 + hf).start()
        messages(phase, j, 0, 4).wait_send()

    def rs_finish(phase, j, store):
        got, _, _, _ = bufs[phase]
        messages(phase, j, 2, 6).wait_recv()
        for k in range(2):
            q, _, _ = ring[phase][k]
            for hf in range(2):
                total = (
                    term(phase, j, k, q, hf, True)[...]
                    + got[turn(got, j), 4 + hf, k].astype(F32)
                    + got[turn(got, j), 3 - hf, k].astype(F32)
                )
                store(k, hf, total)
        messages(phase, j, 4, 6).wait_send()

    def store_t(j):
        def store(k, hf, total):
            t32[turn(t32, j), k, :, pl.ds(hf * CH, CH)] = total
            t16[turn(t16, j), k, :, pl.ds(hf * CH, CH)] = total.astype(BF16)

        return store

    def y_block(phase, j, k, q, hf=None):
        q1 = ring[1][k][0]
        col = core * C + k * CB + (0 if hf is None else hf * CH)
        cols = pl.ds(pl.multiple_of(col, CH), CB if hf is None else CH)
        if phase == 2:
            row = j * R + q1 * R1 + lax.rem(q + side, side) * R2
            return y.at[pl.ds(pl.multiple_of(row, R2), R2), cols]
        row = j * R + lax.rem(q + side, side) * R1
        return y.at[pl.ds(pl.multiple_of(row, R1), R1), cols]

    gsem = {1: (rg1a, rg1b), 2: (rg2a, rg2b)}

    def gather(phase, j, k, m):
        rs = gsem[phase][m // 2]
        q, np_, nm = ring[phase][k]
        dq, hf = ((0, None), (0, None), (-1, 0), (1, 1))[m]
        block = y_block(phase, j, k, q + dq, hf)
        return remote(block, block, sy, rs.at[turn(rs, j)], (np_, nm)[m % 2])

    def gathers(phase, j, late):
        rs = gsem[phase][late]
        size = (R1, R)[phase == 1] // (1 + late)
        block = y.at[pl.ds(pl.multiple_of(j * R, R), size), pl.ds(0, CB)]
        return remote(block, block, sy, rs.at[turn(rs, j)], mate)

    def ag_start(phase, j):
        for m in range(2):
            for k in range(2):
                gather(phase, j, k, m).start()

    def ag_pass(phase, j):
        gathers(phase, j, 0).wait_recv()
        for m in range(2):
            for k in range(2):
                gather(phase, j, k, 2 + m).start()

    def ag_end(phase, j):
        gathers(phase, j, 1).wait_recv()

    def swap(j, k, dq):
        block = y_block(1, j, k, ring[1][k][0] + dq)
        return remote(block, block, sy, rd, mate)

    def stage2(j):
        rs_finish(1, j, store_t(j))
        rs_raw(2, j)

    def stage4(j):
        def store(k, hf, total):
            q2 = ring[2][k][0]
            y_block(2, j, k, q2, hf)[...] = total.astype(BF16)

        rs_finish(2, j, store)
        ag_start(2, j)

    def stage6(j):
        ag_end(2, j)
        ag_start(1, j)

    def stage7(j):
        ag_pass(1, j)
        for dq in (-1, 0, 1):
            for k in range(2):
                swap(j, k, dq).start()

    def stage8(j):
        ag_end(1, j)
        for k in range(2):
            swap(j, k, 2).start()

    stages = (
        None,
        functools.partial(rs_forward, 1),
        stage2,
        functools.partial(rs_forward, 2),
        stage4,
        functools.partial(ag_pass, 2),
        stage6,
        stage7,
        stage8,
    )

    gate_up_first()

    def step(s, carry):
        def run(i):
            j = s - LAGS[i]

            @pl.when(jnp.logical_and(j >= 0, j < nc))
            def _():
                stages[i](j)

        for i in range(len(stages) - 1, 1, -1):
            run(i)

        @pl.when(s + 1 < nc)
        def _():
            gate_up(s + 1)

        run(1)

        @pl.when(s < nc)
        def _():
            @pl.when(s == 0)
            def _():
                wd_own.wait()
                wd_mate.wait()

            down(s)
            rs_raw(1, s)

        return carry

    lax.fori_loop(0, nc + LAGS[-1], step, 0)

    half_y = y.at[:, mate_cols]
    remote(half_y, half_y, sy, rd, mate).wait_recv()
    sent = y.at[pl.ds(0, nc * (R + 3 * (R1 + R2)) // 2), :]
    remote(sent, sent, sy, rd, mate).wait_send()


def _store(y, out, sems):
    size = y.shape[0] // STORES
    copies = [
        pltpu.make_async_copy(y.at[pl.ds(i * size, size), :], out.at[pl.ds(i * size, size), :], sems.at[i])
        for i in range(STORES)
    ]
    for copy in copies:
        copy.start()
    for copy in copies:
        copy.wait()


def _mlp(side, x, w_gate, w_up, w_down):
    rows, depth = x.shape
    ff = w_gate.shape[1]
    width = w_down.shape[1]
    C = width // 2
    R = ROWS
    nc = rows // R
    CB, CH = C // 2, C // 4
    R1, R2 = R // side, R // side // side
    L = LAGS
    dma = pltpu.SemaphoreType.DMA
    y = pl.pallas_call(
        functools.partial(_kernel, side, nc),
        out_shape=pltpu.VMEM((rows, width), BF16),
        in_specs=[pl.BlockSpec(memory_space=pl.ANY)] * 4,
        out_specs=pl.BlockSpec(memory_space=pltpu.VMEM),
        scratch_shapes=[
            pltpu.VMEM((2, depth, ff), BF16),
            pltpu.VMEM((2 * ff, C), BF16),
            pltpu.VMEM((2, R, depth), BF16),
            pltpu.VMEM((4, R, 2 * ff), BF16),
            pltpu.VMEM((L[2], R, C), F32),
            pltpu.VMEM((L[1], R, C), BF16),
            pltpu.VMEM((2 * L[2] - L[1], 6, 2, R1, CH), BF16),
            pltpu.VMEM((2 * L[4] - L[3] - L[2], 6, 2, R2, CH), BF16),
            pltpu.VMEM((L[2] - L[1], 2, 2, R1, CH), BF16),
            pltpu.VMEM((L[4] - L[3], 2, 2, R2, CH), BF16),
            pltpu.VMEM((L[4] - L[2], 2, R1, CB), F32),
            pltpu.VMEM((L[3] - L[2], 2, R1, CB), BF16),
            dma((L[1],)), dma((L[2] - L[1],)), dma((L[2],)), dma((2 * L[2] - L[1],)),
            dma((L[3] - L[2],)), dma((L[4] - L[3],)), dma((L[4] - L[2],)), dma((2 * L[4] - L[3] - L[2],)),
            dma, dma((L[6] - L[4],)), dma((L[6] - L[5] + 2,)), dma((L[8] - L[6],)), dma((L[8] - L[6],)), dma,
            dma((2,)), dma((4,)),
            dma((2,)),
        ],
        compiler_params=pltpu.CompilerParams(
            collective_id=0, has_side_effects=True, vmem_limit_bytes=43 * 1024 * 1024,
        ),
        cost_estimate=pl.CostEstimate(
            flops=6 * rows * depth * ff, bytes_accessed=4 * rows * depth, transcendentals=rows * ff,
        ),
    )(x, w_gate, w_up, w_down)
    return pl.pallas_call(
        _store,
        out_shape=jax.ShapeDtypeStruct((rows, width), BF16),
        in_specs=[pl.BlockSpec(memory_space=pl.ANY)],
        out_specs=pl.BlockSpec(memory_space=pl.ANY),
        scratch_shapes=[dma((STORES,))],
        compiler_params=pltpu.CompilerParams(vmem_limit_bytes=1024 * 1024),
        cost_estimate=pl.CostEstimate(flops=0, bytes_accessed=2 * rows * width, transcendentals=0),
    )(pltpu.with_memory_space_constraint(y, pltpu.VMEM))


def solution(mesh):
    side = math.isqrt(mesh.shape["tp"] // 2)

    return jax.shard_map(
        functools.partial(_mlp, side),
        mesh=mesh,
        in_specs=(P("dp", None), P(None, "tp"), P(None, "tp"), P("tp", None)),
        out_specs=P("dp", None),
        check_vma=False,
    )
```
